32 devices in a mesh: outer: 2 (over y), inner: 4 (over x, core), heads: 4 (over z).
Axes of the slice: x: 2, y: 2, z: 4, core: 2. Of those that a mesh axis runs over, the one named last changes fastest.
Arguments:
- raw_keys: bfloat16 [8, 4096, 8, 128], P(None, ('outer', 'inner'), 'heads'), may hold values from -6 to 6
- raw_values: bfloat16 [8, 4096, 8, 128], P(None, ('outer', 'inner'), 'heads'), may hold values from -6 to 6
- turn_angle: float32 [4096, 64], replicated, may hold values from -3.140625 to 3.140625
Outputs:
- stored_keys: bfloat16 [8, 4096, 8, 128], P(('outer', 'inner'), None, 'heads')
- stored_values: bfloat16 [8, 4096, 8, 128], P(('outer', 'inner'), None, 'heads')
- page_high: bfloat16 [8, 64, 8, 128], P(('outer', 'inner'), None, 'heads')
- page_low: bfloat16 [8, 64, 8, 128], P(('outer', 'inner'), None, 'heads')
The draws below stay inside these ranges and needn't reach their ends.
All inputs are finite; a program needn't handle non-finite values.
Results may differ from the reference program's by a relative error of at most 0.001.
Values may be sent and summed in bfloat16 or wider, within the bound.
A program may use at most 128 MiB of HBM per device.

```python
import jax
import jax.numpy as jnp

BATCH = 8
LENGTH = 4096
KV_HEADS = 8
HEAD_SIZE = 128
HALF_HEAD = 64
PAGE = 64


def block_levels(own_key, extent, shards, smallest, largest):
    factor_of = 1.0
    for axis_at, parts in shards:
        steps = jax.random.uniform(jax.random.fold_in(jax.random.fold_in(own_key, 6), axis_at), (parts,), jnp.float32, smallest / len(shards), largest / len(shards))
        factor_of = factor_of * jnp.repeat(jnp.exp(steps), extent[axis_at] // parts).reshape((-1,) + (1,) * (len(extent) - 1 - axis_at))
    return factor_of


def scatter_about(own_key, shape, deviation, most, split=(), dtype=jnp.bfloat16):
    array = deviation * jax.random.normal(own_key, shape, jnp.float32)
    if split:
        array = array * block_levels(own_key, shape, split, -0.22, 0.18)
    return jnp.clip(array, -most, most).astype(dtype)


def setup_inputs(seed: int = 0) -> dict:
    key_list = jax.random.split(jax.random.key(seed), 4)
    raw_keys = scatter_about(key_list[0], (BATCH, LENGTH, KV_HEADS, HEAD_SIZE), 1.0, 6.0, ((1, 8), (2, 4)))
    raw_values = scatter_about(key_list[1], (BATCH, LENGTH, KV_HEADS, HEAD_SIZE), 1.0, 6.0, ((1, 8), (2, 4)))
    turn_angle = jnp.clip(jax.random.uniform(key_list[2], (LENGTH, HALF_HEAD), jnp.float32, -3.140625, 3.140625), -3.140625, 3.140625)
    return {"raw_keys": raw_keys, "raw_values": raw_values, "turn_angle": turn_angle}


def turn_pairs(vectors, angle):
    half = vectors.shape[-1] // 2
    cosine, sine = jnp.cos(angle)[None, :, None, :], jnp.sin(angle)[None, :, None, :]
    first, second = vectors[..., :half], vectors[..., half:]
    return jnp.concatenate([first * cosine - second * sine, second * cosine + first * sine], axis=-1)


def prepare_keys(plain_keys, angle):
    wide_keys = plain_keys.astype(jnp.float32)
    return turn_pairs(wide_keys, angle)


def reference(raw_keys, raw_values, turn_angle):
    turned_keys = prepare_keys(raw_keys, turn_angle)
    narrow_keys = turned_keys.astype(jnp.bfloat16)
    page_view = narrow_keys.reshape(BATCH, LENGTH // PAGE, PAGE, KV_HEADS, HEAD_SIZE)
    page_high = jnp.max(page_view, axis=2)
    page_low = jnp.min(page_view, axis=2)
    stored_keys = narrow_keys
    stored_values = raw_values
    return stored_keys, stored_values, page_high, page_low
```

```python
import functools

import jax
import jax.numpy as jnp
from jax import lax
from jax.experimental import pallas as pl
from jax.experimental.pallas import tpu as pltpu
from jax.sharding import PartitionSpec as P

PAGE = 64
MESH = pl.DeviceIdType.MESH

FIRST = (("YX", "kv"),)
EVEN = (("Dd", "kv"), ("Yy", "kv"), ("c", "k"), ("Xx", "kv"), ("c", "v"))
ODD = (("xy", "kv"), ("c", "k"), ("Dd", "kv"), ("c", "v"))
TURNS = "YXDdxyc"


def offsets(outer, inner):
    cores = 2 if inner % 2 == 0 else 1
    chips = inner // cores
    steps = [
        (do, dx, dc)
        for dc in range(cores)
        for do in range(outer)
        for dx in range(chips)
        if (do, dx, dc) != (0, 0, 0)
    ]
    return cores, chips, steps


def kind(step):
    name = ("c", "x", "y", "d")[(step[1] != 0) + 2 * (step[0] != 0)]
    return name if step[2] or name == "c" else name.upper()


def queue(steps, spec):
    return [
        (j, tensor)
        for kinds, tensors in spec
        for tensor in tensors
        for name in kinds
        for j, step in enumerate(steps)
        if kind(step) == name
    ]


def kernel(
    outer, inner, heads,
    keys, values, angle,
    out_keys, out_values, out_high, out_low,
    landed, angles, table, wide, turned, bound,
    send_k, recv_k, send_v, recv_v, ready, local,
):
    group = outer * inner
    batch, rows, size = keys.shape
    own = batch // group
    length = rows // heads
    half = size // 2
    pages = length // PAGE
    cores, chips, steps = offsets(outer, inner)
    o, i = lax.axis_index("outer"), lax.axis_index("inner")
    x, c = i // cores, i % cores
    me = o * inner + i

    def partner(step, sign):
        do, dx, dc = step
        po = (o + sign * do + outer) % outer
        pi = (x + sign * dx + chips) % chips * cores + (c + sign * dc + cores) % cores
        return po, pi

    def tell(sem, kinds):
        for step in steps:
            if kind(step) in kinds:
                po, pi = partner(step, -1)
                pl.semaphore_signal(
                    sem, inc=1, device_id={"outer": po, "inner": pi}, device_id_type=MESH
                )

    square = (outer, chips, cores) == (2, 2, 2)
    barrier = pltpu.get_barrier_semaphore()
    if square:
        pl.when((c == 1) & (o + x < 2))(lambda: tell(barrier, "XY"))
        pl.when(c == 1)(lambda: tell(barrier, "c"))
    else:
        tell(barrier, "cxydXYD")

    get_angles = pltpu.make_async_copy(angle, angles, local.at[0])
    mine = pl.ds(pl.multiple_of(me * rows, rows), rows)
    own_keys = pltpu.make_async_copy(
        keys.at[pl.ds(me * own, own)], landed.at[:, mine], local.at[1]
    )
    own_values = pltpu.make_async_copy(
        values.at[pl.ds(me * own, own)], out_values.at[:, mine], local.at[2]
    )

    copies = {}
    for j, step in enumerate(steps):
        po, pi = partner(step, 1)
        theirs = pl.ds((po * inner + pi) * own, own)
        for tensor, src, dst, send, recv in (
            ("k", keys, landed, send_k, recv_k),
            ("v", values, out_values, send_v, recv_v),
        ):
            copies[j, tensor] = pltpu.make_async_remote_copy(
                src_ref=src.at[theirs],
                dst_ref=dst.at[:, mine],
                send_sem=send.at[j],
                recv_sem=recv.at[j],
                device_id={"outer": po, "inner": pi},
                device_id_type=MESH,
            )

    def issue(spec, names="cxydXYD"):
        for j, tensor in queue(steps, spec):
            if kind(steps[j]) in names:
                copies[j, tensor].start()

    if square:
        pl.semaphore_wait(barrier, 1 + c * ((o + x + 1) % 2))

        @pl.when((c == 1) & (o + x == 2))
        def _():
            tell(ready.at[0], "XY")

        @pl.when((c == 1) & (o + x != 1))
        def _():
            issue(FIRST)

        for near, far, at in (("X", "Y", 1), ("Y", "X", 0)):
            @pl.when((c == 1) & (o + x == 1) & (x == at))
            def _(near=near, far=far):
                issue(FIRST, near)
                pl.semaphore_wait(ready.at[0], 1)
                issue(FIRST, far)

        @pl.when(c == 1)
        def _():
            pl.semaphore_wait(ready.at[1], 1)
            for stage in (2, 3):
                tell(ready.at[stage], "XY")
                pl.semaphore_wait(ready.at[stage], 2)
            tell(ready.at[1], "c")

        @pl.when(c == 0)
        def _():
            tell(ready.at[1], "c")
            pl.semaphore_wait(ready.at[1], 1)
    else:
        pl.semaphore_wait(barrier, len(steps))
        pl.when(c == 1)(lambda: issue(FIRST))

    get_angles.start()
    own_keys.start()
    own_values.start()
    pl.when(c == 0)(lambda: issue(EVEN))
    pl.when(c == 1)(lambda: issue(ODD))

    get_angles.wait()

    def fill(p, carry):
        at = pl.ds(pl.multiple_of(p * size, size), size)
        a = angles[:, at]
        table[at] = jnp.concatenate([jnp.cos(a), jnp.sin(a)], axis=0).T
        return carry

    lax.fori_loop(0, table.shape[0] // size, fill, 0)

    def turn(source):
        for n in range(own):
            def page(p, carry):
                at = pl.multiple_of(source * length + p * PAGE, PAGE)
                tab = table[pl.ds(at, PAGE)]
                swap = pltpu.roll(tab, half, 1)
                low_half = lax.broadcasted_iota(jnp.int32, tab.shape, 1) < half
                cosine = jnp.where(low_half, tab, swap)
                sine = jnp.where(low_half, -swap, tab)
                at_rows = pl.ds(pl.multiple_of(at * heads, PAGE * heads), PAGE * heads)
                wide[...] = landed[n, at_rows].astype(jnp.float32)
                for h in range(heads):
                    v = wide[pl.ds(h, PAGE, stride=heads)]
                    y = v * cosine + pltpu.roll(v, half, 1) * sine
                    turned[pl.ds(h, PAGE, stride=heads)] = y
                    bound[0, pl.ds(p * heads + h, 1)] = jnp.max(y, axis=0, keepdims=True)
                    bound[1, pl.ds(p * heads + h, 1)] = jnp.min(y, axis=0, keepdims=True)
                out_keys[n, at_rows] = turned[...].astype(out_keys.dtype)
                return carry

            lax.fori_loop(0, pages, page, 0)
            at_pages = pl.ds(pl.multiple_of(source * pages * heads, pages * heads), pages * heads)
            out_high[n, at_pages] = bound[0].astype(out_high.dtype)
            out_low[n, at_pages] = bound[1].astype(out_low.dtype)

    own_keys.wait()
    turn(me)
    for j, _ in queue(steps, ((TURNS, "k"),)):
        copies[j, "k"].wait_recv()
        po, pi = partner(steps[j], -1)
        turn(po * inner + pi)
    own_values.wait()
    for j in range(len(steps)):
        copies[j, "v"].wait_recv()
    for copy in copies.values():
        copy.wait_send()


def in_hbm(array):
    return pltpu.with_memory_space_constraint(array, pltpu.HBM)


def store(*refs):
    count = len(refs) // 2
    sems = refs[-1]
    copies = [
        pltpu.make_async_copy(refs[k], refs[count + k], sems.at[k]) for k in range(count)
    ]
    for copy in copies:
        copy.start()
    for copy in copies:
        copy.wait()


def per_device(outer, inner, raw_keys, raw_values, turn_angle):
    batch, length, heads, size = raw_keys.shape
    group = outer * inner
    own, rows, pages = batch // group, length * heads, length // PAGE
    bf16, f32 = jnp.bfloat16, jnp.float32
    scratch_bytes = group * length * size * (2 * own * heads + 8) + 2**22
    outs = pl.pallas_call(
        functools.partial(kernel, outer, inner, heads),
        out_shape=(
            pltpu.VMEM((own, group * rows, size), bf16),
            pltpu.VMEM((own, group * rows, size), bf16),
            pltpu.VMEM((own, group * pages * heads, size), bf16),
            pltpu.VMEM((own, group * pages * heads, size), bf16),
        ),
        in_specs=[pl.BlockSpec(memory_space=pltpu.HBM)] * 3,
        out_specs=[pl.BlockSpec(memory_space=pltpu.VMEM)] * 4,
        scratch_shapes=[
            pltpu.VMEM((own, group * rows, size), bf16),
            pltpu.VMEM((turn_angle.shape[1], turn_angle.shape[0]), f32),
            pltpu.VMEM((turn_angle.shape[0], size), f32),
            pltpu.VMEM((PAGE * heads, size), f32),
            pltpu.VMEM((PAGE * heads, size), f32),
            pltpu.VMEM((2, pages * heads, size), f32),
            pltpu.SemaphoreType.DMA((group,)),
            pltpu.SemaphoreType.DMA((group,)),
            pltpu.SemaphoreType.DMA((group,)),
            pltpu.SemaphoreType.DMA((group,)),
            pltpu.SemaphoreType.REGULAR((4,)),
            pltpu.SemaphoreType.DMA((3,)),
        ],
        compiler_params=pltpu.CompilerParams(
            collective_id=0, has_side_effects=True, vmem_limit_bytes=scratch_bytes
        ),
    )(
        in_hbm(raw_keys.reshape(batch, rows, size)),
        in_hbm(raw_values.reshape(batch, rows, size)),
        in_hbm(turn_angle.T),
    )
    keys, values, high, low = pl.pallas_call(
        store,
        out_shape=[jax.ShapeDtypeStruct(out.shape, out.dtype) for out in outs],
        in_specs=[pl.BlockSpec(memory_space=pltpu.VMEM)] * 4,
        out_specs=[pl.BlockSpec(memory_space=pltpu.HBM)] * 4,
        scratch_shapes=[pltpu.SemaphoreType.DMA((4,))],
        compiler_params=pltpu.CompilerParams(vmem_limit_bytes=2**20),
    )(*outs)
    return (
        keys.reshape(own, group * length, heads, size),
        values.reshape(own, group * length, heads, size),
        high.reshape(own, group * pages, heads, size),
        low.reshape(own, group * pages, heads, size),
    )


def solution(mesh):
    moved = P(None, ("outer", "inner"), "heads", None)
    whole = P(("outer", "inner"), None, "heads", None)
    return jax.shard_map(
        functools.partial(per_device, mesh.shape["outer"], mesh.shape["inner"]),
        mesh=mesh,
        in_specs=(moved, moved, P()),
        out_specs=(whole,) * 4,
        check_vma=False,
    )
```

```python
import functools

import jax
import jax.numpy as jnp
from jax import lax
from jax.experimental import pallas as pl
from jax.experimental.pallas import tpu as pltpu
from jax.sharding import PartitionSpec as P

PAGE = 64
MESH = pl.DeviceIdType.MESH

FIRST = (("YX", "k"),)
EVEN = (("dy", "kv"), ("c", "k"), ("xY", "kv"), ("D", "kv"), ("X", "kv"), ("c", "v"))
ODD = (("xy", "v"), ("c", "k"), ("D", "k"), ("d", "kv"), ("c", "v"))
MIDDLE = (("xy", "k"),)
LAST = (("DYX", "v"),)
ALL = (("cXYxy", "k"), ("cXYxy", "v"), ("Dd", "k"), ("Dd", "v"))
TURNS = "dYyXxDc"


def offsets(outer, inner):
    cores = 2 if inner % 2 == 0 else 1
    chips = inner // cores
    steps = [
        (do, dx, dc)
        for dc in range(cores)
        for do in range(outer)
        for dx in range(chips)
        if (do, dx, dc) != (0, 0, 0)
    ]
    return cores, chips, steps


def is_square(outer, inner):
    cores, chips, _ = offsets(outer, inner)
    return (outer, chips, cores) == (2, 2, 2)


def kind(step):
    name = ("c", "x", "y", "d")[(step[1] != 0) + 2 * (step[0] != 0)]
    return name if step[2] or name == "c" else name.upper()


def queue(steps, spec):
    return [
        (j, tensor)
        for kinds, tensors in spec
        for tensor in tensors
        for name in kinds
        for j, step in enumerate(steps)
        if kind(step) == name
    ]


def kernel(
    outer, inner, heads,
    keys, values, angle,
    out_keys, out_values, out_high, out_low,
    landed, angles, table, wide, turned, bound,
    send_k, recv_k, send_v, recv_v, ready, local,
):
    group = outer * inner
    batch, rows, size = keys.shape
    own = batch // group
    length = rows // heads
    half = size // 2
    pages = length // PAGE
    cores, chips, steps = offsets(outer, inner)
    o, i = lax.axis_index("outer"), lax.axis_index("inner")
    x, c = i // cores, i % cores
    me = o * inner + i

    def partner(step, sign):
        do, dx, dc = step
        po = (o + sign * do + outer) % outer
        pi = (x + sign * dx + chips) % chips * cores + (c + sign * dc + cores) % cores
        return po, pi

    def tell(sem, kinds):
        for step in steps:
            if kind(step) in kinds:
                po, pi = partner(step, -1)
                pl.semaphore_signal(
                    sem, inc=1, device_id={"outer": po, "inner": pi}, device_id_type=MESH
                )

    square = is_square(outer, inner)
    barrier = pltpu.get_barrier_semaphore()
    if square:
        pl.when((c == 1) & (o + x < 2))(lambda: tell(barrier, "XY"))
        pl.when(c == 1)(lambda: tell(barrier, "c"))
    else:
        tell(barrier, "cxydXYD")

    get_angles = pltpu.make_async_copy(angle, angles, local.at[0])
    mine = pl.ds(pl.multiple_of(me * rows, rows), rows)
    own_keys = pltpu.make_async_copy(
        keys.at[pl.ds(me * own, own)], landed.at[:, mine], local.at[1]
    )
    own_values = pltpu.make_async_copy(
        values.at[pl.ds(me * own, own)], out_values.at[:, mine], local.at[2]
    )

    copies = {}
    for j, step in enumerate(steps):
        po, pi = partner(step, 1)
        theirs = pl.ds((po * inner + pi) * own, own)
        for tensor, src, dst, send, recv in (
            ("k", keys, landed, send_k, recv_k),
            ("v", values, out_values, send_v, recv_v),
        ):
            copies[j, tensor] = pltpu.make_async_remote_copy(
                src_ref=src.at[theirs],
                dst_ref=dst.at[:, mine],
                send_sem=send.at[j],
                recv_sem=recv.at[j],
                device_id={"outer": po, "inner": pi},
                device_id_type=MESH,
            )

    def issue(spec, names="cxydXYD"):
        for j, tensor in queue(steps, spec):
            if kind(steps[j]) in names:
                copies[j, tensor].start()

    if square:
        pl.semaphore_wait(barrier, 1 + c * ((o + x + 1) % 2))

        @pl.when((c == 1) & (o + x == 2))
        def _():
            tell(ready.at[0], "XY")

        @pl.when((c == 1) & (o + x != 1))
        def _():
            issue(FIRST)

        for near, far, at in (("X", "Y", 1), ("Y", "X", 0)):
            @pl.when((c == 1) & (o + x == 1) & (x == at))
            def _(near=near, far=far):
                issue(FIRST, near)
                pl.semaphore_wait(ready.at[0], 1)
                issue(FIRST, far)

        @pl.when(c == 1)
        def _():
            pl.semaphore_wait(ready.at[1], 1)
            for stage in (2, 3):
                tell(ready.at[stage], "XY")
                pl.semaphore_wait(ready.at[stage], 2)
                if stage == 2:
                    issue(MIDDLE)
            tell(ready.at[1], "c")

        @pl.when(c == 0)
        def _():
            tell(ready.at[1], "c")
            pl.semaphore_wait(ready.at[1], 1)
    else:
        pl.semaphore_wait(barrier, len(steps))

    get_angles.start()
    own_keys.start()
    own_values.start()
    if square:
        pl.when(c == 0)(lambda: issue(EVEN))
        pl.when(c == 1)(lambda: issue(ODD))
    else:
        issue(ALL)

    get_angles.wait()

    def fill(p, carry):
        at = pl.ds(pl.multiple_of(p * size, size), size)
        a = angles[:, at]
        table[at] = jnp.concatenate([jnp.cos(a), jnp.sin(a)], axis=0).T
        return carry

    lax.fori_loop(0, table.shape[0] // size, fill, 0)

    def turn(source):
        for n in range(own):
            def page(p, carry):
                at = pl.multiple_of(source * length + p * PAGE, PAGE)
                tab = table[pl.ds(at, PAGE)]
                swap = pltpu.roll(tab, half, 1)
                low_half = lax.broadcasted_iota(jnp.int32, tab.shape, 1) < half
                cosine = jnp.where(low_half, tab, swap)
                sine = jnp.where(low_half, -swap, tab)
                at_rows = pl.ds(pl.multiple_of(at * heads, PAGE * heads), PAGE * heads)
                wide[...] = landed[n, at_rows].astype(jnp.float32)
                for h in range(heads):
                    v = wide[pl.ds(h, PAGE, stride=heads)]
                    y = v * cosine + pltpu.roll(v, half, 1) * sine
                    turned[pl.ds(h, PAGE, stride=heads)] = y
                    bound[0, pl.ds(p * heads + h, 1)] = jnp.max(y, axis=0, keepdims=True)
                    bound[1, pl.ds(p * heads + h, 1)] = jnp.min(y, axis=0, keepdims=True)
                out_keys[n, at_rows] = turned[...].astype(out_keys.dtype)
                return carry

            lax.fori_loop(0, pages, page, 0)
            at_pages = pl.ds(pl.multiple_of(source * pages * heads, pages * heads), pages * heads)
            out_high[n, at_pages] = bound[0].astype(out_high.dtype)
            out_low[n, at_pages] = bound[1].astype(out_low.dtype)

    own_keys.wait()
    turn(me)
    for j, _ in queue(steps, ((TURNS, "k"),)):
        copies[j, "k"].wait_recv()
        po, pi = partner(steps[j], -1)
        turn(po * inner + pi)
    own_values.wait()
    late = queue(steps, LAST) if square else []
    sent = [n for n in copies if n not in late]
    for j, tensor in sent:
        if tensor == "v":
            copies[j, tensor].wait_recv()
    for n in sent:
        copies[n].wait_send()

    @pl.when(c == 0)
    def _():
        for n in late:
            copies[n].wait_recv()
            copies[n].wait_send()


def last_kernel(outer, inner, values, after, arrived, send, recv):
    own = arrived.shape[1]
    cores, chips, steps = offsets(outer, inner)
    o, i = lax.axis_index("outer"), lax.axis_index("inner")
    x, c = i // cores, i % cores
    targets = []
    for j, _ in queue(steps, LAST):
        do, dx, dc = steps[j]
        targets.append(((o + do) % outer, (x + dx) % chips * cores + c))

    @pl.when(c == 1)
    def _():
        barrier = pltpu.get_barrier_semaphore()
        for po, pi in targets:
            pl.semaphore_signal(
                barrier, inc=1, device_id={"outer": po, "inner": pi}, device_id_type=MESH
            )
        pl.semaphore_wait(barrier, len(targets))
        copies = [
            pltpu.make_async_remote_copy(
                src_ref=values.at[pl.ds((po * inner + pi) * own, own)],
                dst_ref=arrived.at[n],
                send_sem=send.at[n],
                recv_sem=recv.at[n],
                device_id={"outer": po, "inner": pi},
                device_id_type=MESH,
            )
            for n, (po, pi) in enumerate(targets)
        ]
        for copy in copies:
            copy.start()
        for copy in copies:
            copy.wait()


def in_hbm(array):
    return pltpu.with_memory_space_constraint(array, pltpu.HBM)


def store(outer, inner, *refs):
    count = len(refs) // 2
    sems = refs[-1]
    square = is_square(outer, inner)
    always = [
        pltpu.make_async_copy(refs[k], refs[count + k], sems.at[k])
        for k in range(count)
        if k != 1 or not square
    ]
    if not square:
        for copy in always:
            copy.start()
        for copy in always:
            copy.wait()
        return

    group = outer * inner
    rows = refs[1].shape[1] // group
    o, i = lax.axis_index("outer"), lax.axis_index("inner")
    x, c = i // 2, i % 2
    steps = offsets(outer, inner)[2]
    waiting = [steps[j] for j, _ in queue(steps, LAST)]
    parts = []
    for do, dx, dc in [(0, 0, 0)] + steps:
        origin = (o + do) % 2 * inner + (x + dx) % 2 * 2 + (c + dc) % 2
        at = pl.ds(pl.multiple_of(origin * rows, rows), rows)
        late = (do, dx, dc) in waiting
        parts.append((late, pltpu.make_async_copy(
            refs[1].at[:, at], refs[count + 1].at[:, at], sems.at[count + len(parts)]
        )))
    always += [copy for late, copy in parts if not late]
    for copy in always:
        copy.start()

    @pl.when(c == 0)
    def _():
        for late, copy in parts:
            if late:
                copy.start()
        for late, copy in parts:
            if late:
                copy.wait()

    for copy in always:
        copy.wait()


def store_last(outer, inner, arrived, before, values, sems):
    rows = arrived.shape[2]
    o, i = lax.axis_index("outer"), lax.axis_index("inner")
    x, c = i // 2, i % 2

    @pl.when(c == 1)
    def _():
        copies = []
        steps = offsets(outer, inner)[2]
        for n, (j, _) in enumerate(queue(steps, LAST)):
            do, dx, dc = steps[j]
            origin = (o + do) % 2 * inner + (x + dx) % 2 * 2 + c
            at = pl.ds(pl.multiple_of(origin * rows, rows), rows)
            copies.append(pltpu.make_async_copy(arrived.at[n], values.at[:, at], sems.at[n]))
        for copy in copies:
            copy.start()
        for copy in copies:
            copy.wait()


def per_device(outer, inner, raw_keys, raw_values, turn_angle):
    batch, length, heads, size = raw_keys.shape
    group = outer * inner
    own, rows, pages = batch // group, length * heads, length // PAGE
    bf16, f32 = jnp.bfloat16, jnp.float32
    scratch_bytes = group * length * size * (2 * own * heads + 8) + 2**22
    outs = pl.pallas_call(
        functools.partial(kernel, outer, inner, heads),
        out_shape=(
            pltpu.VMEM((own, group * rows, size), bf16),
            pltpu.VMEM((own, group * rows, size), bf16),
            pltpu.VMEM((own, group * pages * heads, size), bf16),
            pltpu.VMEM((own, group * pages * heads, size), bf16),
        ),
        in_specs=[pl.BlockSpec(memory_space=pltpu.HBM)] * 3,
        out_specs=[pl.BlockSpec(memory_space=pltpu.VMEM)] * 4,
        scratch_shapes=[
            pltpu.VMEM((own, group * rows, size), bf16),
            pltpu.VMEM((turn_angle.shape[1], turn_angle.shape[0]), f32),
            pltpu.VMEM((turn_angle.shape[0], size), f32),
            pltpu.VMEM((PAGE * heads, size), f32),
            pltpu.VMEM((PAGE * heads, size), f32),
            pltpu.VMEM((2, pages * heads, size), f32),
            pltpu.SemaphoreType.DMA((group,)),
            pltpu.SemaphoreType.DMA((group,)),
            pltpu.SemaphoreType.DMA((group,)),
            pltpu.SemaphoreType.DMA((group,)),
            pltpu.SemaphoreType.REGULAR((4,)),
            pltpu.SemaphoreType.DMA((3,)),
        ],
        compiler_params=pltpu.CompilerParams(
            collective_id=0, has_side_effects=True, vmem_limit_bytes=scratch_bytes
        ),
    )(
        in_hbm(raw_keys.reshape(batch, rows, size)),
        in_hbm(raw_values.reshape(batch, rows, size)),
        in_hbm(turn_angle.T),
    )
    keys, values, high, low = pl.pallas_call(
        functools.partial(store, outer, inner),
        out_shape=[pltpu.HBM(out.shape, out.dtype) for out in outs],
        in_specs=[pl.BlockSpec(memory_space=pltpu.VMEM)] * 4,
        out_specs=[pl.BlockSpec(memory_space=pltpu.HBM)] * 4,
        scratch_shapes=[pltpu.SemaphoreType.DMA((4 + group,))],
        compiler_params=pltpu.CompilerParams(vmem_limit_bytes=2**20),
    )(*outs)
    if is_square(outer, inner):
        late = len(queue(offsets(outer, inner)[2], LAST))
        arrived = pl.pallas_call(
            functools.partial(last_kernel, outer, inner),
            out_shape=pltpu.VMEM((late, own, rows, size), bf16),
            in_specs=[pl.BlockSpec(memory_space=pltpu.HBM)] * 2,
            out_specs=pl.BlockSpec(memory_space=pltpu.VMEM),
            scratch_shapes=[pltpu.SemaphoreType.DMA((late,))] * 2,
            compiler_params=pltpu.CompilerParams(
                collective_id=1, has_side_effects=True, vmem_limit_bytes=2**20 + late * own * rows * size * 2
            ),
        )(in_hbm(raw_values.reshape(batch, rows, size)), in_hbm(low))
        values = pl.pallas_call(
            functools.partial(store_last, outer, inner),
            out_shape=pltpu.HBM(values.shape, values.dtype),
            in_specs=[
                pl.BlockSpec(memory_space=pltpu.VMEM),
                pl.BlockSpec(memory_space=pltpu.HBM),
            ],
            out_specs=pl.BlockSpec(memory_space=pltpu.HBM),
            scratch_shapes=[pltpu.SemaphoreType.DMA((late,))],
            input_output_aliases={1: 0},
            compiler_params=pltpu.CompilerParams(vmem_limit_bytes=2**20),
        )(arrived, values)
    return (
        keys.reshape(own, group * length, heads, size),
        values.reshape(own, group * length, heads, size),
        high.reshape(own, group * pages, heads, size),
        low.reshape(own, group * pages, heads, size),
    )


def solution(mesh):
    moved = P(None, ("outer", "inner"), "heads", None)
    whole = P(("outer", "inner"), None, "heads", None)
    return jax.shard_map(
        functools.partial(per_device, mesh.shape["outer"], mesh.shape["inner"]),
        mesh=mesh,
        in_specs=(moved, moved, P()),
        out_specs=(whole,) * 4,
        check_vma=False,
    )
```
